128 devices in a mesh: sub: 32 (over y, x, core), grp: 4 (over z).
Axes of the slice: x: 4, y: 4, z: 4, core: 2. Of those that a mesh axis runs over, the one named last changes fastest.
Arguments:
- coupling: float32 [128, 2, 256, 8192], P(('sub', 'grp')), may hold values from -6 to 6
- sketch_matrix: float32 [64, 8192], replicated, may hold values from -0.0625 to 0.0625
- block_rows: int32 [128, 2], P(('sub', 'grp')), may hold values from 128 to 256
- members: int32 [32, 8], replicated, may hold values from 0 to 255, as said below
Outputs:
- bases: float32 [32, 16384], P('sub', 'grp')
- projections: float32 [128, 2, 64, 8192], P(('sub', 'grp'))
The draws below stay inside these ranges and needn't reach their ends.
Inputs may be any that keep to these rules, and one draw needn't show every extreme that they name: `members`: every block number 2 s + k, with s below 128 and k 0 or 1, stands exactly once in the table.
All inputs are finite; a program needn't handle non-finite values.
Results may differ from the reference program's by a relative error of at most 0.000094.
Values sent between devices are 32-bit elements; how exact they have to be, the bound alone decides.
A program may use at most 128 MiB of HBM per device.

```python
import jax
import jax.numpy as jnp
from jax import lax

COLS = 8192
SKETCH = 64
SHARERS = 8
ROWS = 256
SUBDOMAINS = 128
INTERFACES = 32


def draw_members(key, part):
    order = jax.random.permutation(key, 2 * SUBDOMAINS)
    return order.astype(jnp.int32).reshape(INTERFACES, SHARERS)


def touch_ends(drawn, stream_key, low, top_value):
    shape = drawn.shape
    index_at = [jax.random.randint(jax.random.fold_in(stream_key, axis), (), 0, shape[axis]) for axis in range(len(shape))]
    drawn = drawn.at[tuple(index_at)].set(low)
    longest = shape.index(max(shape))
    index_at[longest] = (index_at[longest] + 1) % shape[longest]
    return drawn.at[tuple(index_at)].set(top_value)


def steps_of(rng, extent, split, low, largest):
    def one(axis_at, blocks):
        draws = jax.random.uniform(jax.random.fold_in(jax.random.fold_in(rng, 6), axis_at), (blocks,), jnp.float32, low / len(split), largest / len(split))
        return jnp.repeat(jnp.exp(draws), extent[axis_at] // blocks).reshape((-1,) + (1,) * (len(extent) - axis_at - 1))

    factor_of = one(*split[0])
    for cut in split[1:]:
        factor_of = factor_of * one(*cut)
    return factor_of


def bell_draw(own_key, extent, width, bound, pieces=(), held_as=jnp.bfloat16):
    loudness = steps_of(own_key, extent, pieces, -0.22, 0.18) if pieces else 1.0
    result = jax.random.normal(own_key, extent, jnp.float32) * width * loudness
    return jnp.minimum(jnp.maximum(result, -bound), bound).astype(held_as)


def setup_inputs(seed: int = 0) -> dict:
    key_list = jax.random.split(jax.random.key(seed), 5)
    coupling = bell_draw(key_list[0], (SUBDOMAINS, 2, ROWS, COLS), 1.0, 6.0, ((0, 128),), jnp.float32)
    sketch_matrix = bell_draw(key_list[1], (SKETCH, COLS), COLS ** -0.5, 0.0625, (), jnp.float32)
    block_rows = touch_ends(jax.random.randint(key_list[2], (SUBDOMAINS, 2), ROWS // 2, ROWS + 1), jax.random.fold_in(key_list[2], 1), ROWS // 2, ROWS).astype(jnp.int32)
    members = draw_members(jax.random.fold_in(key_list[4], 71), 0)
    return dict(coupling=coupling, sketch_matrix=sketch_matrix, block_rows=block_rows, members=members)


def reference(coupling, sketch_matrix, block_rows, members):
    positions = jnp.arange(ROWS, dtype=jnp.int32)
    row_mask = (positions[None, None, :] < block_rows[:, :, None]).astype(jnp.float32)

    def sketch_one(blocks):
        return jnp.einsum('krn,cn->krc', blocks, sketch_matrix, precision=lax.Precision.HIGHEST)
    sketches = lax.map(sketch_one, coupling) * row_mask[:, :, :, None]
    flat_sketches = sketches.reshape(2 * SUBDOMAINS, ROWS, SKETCH)
    interface_sum = jnp.sum(flat_sketches[members], axis=1)
    gram_total = jnp.einsum('irc,ird->icd', interface_sum, interface_sum, precision=lax.Precision.HIGHEST)
    factor = jnp.linalg.cholesky(gram_total)
    identity = jnp.eye(SKETCH, dtype=jnp.float32)
    inverse = jax.vmap(lambda single: jax.scipy.linalg.solve_triangular(single, identity, lower=True))(factor)
    bases = jnp.einsum('irc,idc->ird', interface_sum, inverse, precision=lax.Precision.HIGHEST)
    owner_of = jnp.zeros((2 * SUBDOMAINS,), jnp.int32).at[members.reshape(-1)].set(jnp.arange(INTERFACES * SHARERS, dtype=jnp.int32) // SHARERS)
    chosen = bases[owner_of].reshape(SUBDOMAINS, 2, ROWS, SKETCH) * row_mask[:, :, :, None]

    def project_one(pair):
        return jnp.einsum('krc,krn->kcn', pair[1], pair[0], precision=lax.Precision.HIGHEST)
    projections = lax.map(project_one, (coupling, chosen))
    return (bases.reshape(INTERFACES, ROWS * SKETCH), projections)
```

```python
import functools

import jax
import jax.numpy as jnp
from jax import lax
from jax.experimental import pallas as pl
from jax.experimental.pallas import tpu as pltpu
from jax.sharding import PartitionSpec as P

MESH = pl.DeviceIdType.MESH
F32 = jnp.float32
BF16 = jnp.bfloat16
LANES = 128
SIDE = 4
RING = [(dy, dx) for dy in range(SIDE) for dx in range(SIDE)]
FAR_FIRST = sorted(range(1, 16), key=lambda r: -sum(min(d, SIDE - d) for d in RING[r]))
NEAR_FIRST = FAR_FIRST[::-1]


def split_two(x):
    high = x.astype(BF16)
    return high, (x - high.astype(F32)).astype(BF16)


def sketch_kernel(c_hbm, s_hbm, rows_ref, out_ref, cbuf, sbuf, sw, pairs, csem, ssem):
    parts, _, part_rows, cols = cbuf.shape
    width = sbuf.shape[0]
    s_copy = pltpu.make_async_copy(s_hbm, sbuf, ssem)
    s_copy.start()

    def load(t, k):
        return pltpu.make_async_copy(
            c_hbm.at[0, k, pl.ds(t * part_rows, part_rows), :], cbuf.at[t, k], csem.at[t, k]
        )

    for t in range(parts):
        for k in range(2):
            load(t, k).start()
    sw[2 * width :, :] = jnp.zeros((256 - 2 * width, cols), BF16)
    s_copy.wait()
    for n in range(0, cols, 1024):
        high, low = split_two(sbuf[:, n : n + 1024])
        sw[:width, n : n + 1024] = high
        sw[width : 2 * width, n : n + 1024] = low

    def body(acc0, acc1):
        accs = (acc0, acc1)
        for a in accs:
            pltpu.matmul_pop(a)

        def quarter(t, carry):
            for k in range(2):
                load(t, k).wait()
            for j in range(cols // 512):
                for m in range(2):
                    n = (2 * j + m) * 256
                    pltpu.matmul_push_rhs(
                        sw[:, n : n + 256], staging_register=0, mxu_index=m, transpose=True
                    )
                    x = jnp.concatenate([cbuf[t, k, :, n : n + 256] for k in range(2)], axis=0)
                    high, low = split_two(x)
                    pltpu.matmul_acc_lhs(accs[m], high, load_staged_rhs=0)
                    pltpu.matmul_acc_lhs(accs[m], low)
            total = pltpu.matmul_pop(acc0)[:, :LANES] + pltpu.matmul_pop(acc1)[:, :LANES]
            total = total + pltpu.roll(total, LANES // 2, 1)
            spot = lax.broadcasted_iota(jnp.int32, (part_rows, LANES), 0) + t * part_rows
            left = lax.broadcasted_iota(jnp.int32, (part_rows // 2, LANES), 1) < LANES // 2
            for k in range(2):
                live = total[k * part_rows : (k + 1) * part_rows]
                pairs[k] = jnp.where(spot < rows_ref[0, k], live, 0.0)
                even = pairs[k, pl.ds(0, part_rows // 2, stride=2), :]
                odd = pairs[k, pl.ds(1, part_rows // 2, stride=2), :]
                out_ref[t, k] = jnp.where(left, even, odd)
            return carry

        lax.fori_loop(0, parts, quarter, 0)

    pl.run_scoped(
        body, pltpu.ACC(0)((2 * part_rows, 256), F32), pltpu.ACC(1)((2 * part_rows, 256), F32)
    )


def sketch_call(coupling, sketch_matrix, block_rows):
    width, cols = sketch_matrix.shape
    return pl.pallas_call(
        sketch_kernel,
        out_shape=jax.ShapeDtypeStruct((4, 2, 32, LANES), F32),
        in_specs=[
            pl.BlockSpec(memory_space=pl.ANY),
            pl.BlockSpec(memory_space=pl.ANY),
            pl.BlockSpec(memory_space=pltpu.SMEM),
        ],
        out_specs=pl.BlockSpec(memory_space=pltpu.VMEM),
        scratch_shapes=[
            pltpu.VMEM((4, 2, 64, cols), F32),
            pltpu.VMEM((width, cols), F32),
            pltpu.VMEM((256, cols), BF16),
            pltpu.VMEM((2, 64, LANES), F32),
            pltpu.SemaphoreType.DMA((4, 2)),
            pltpu.SemaphoreType.DMA,
        ],
        compiler_params=pltpu.CompilerParams(vmem_limit_bytes=40 << 20),
        name="sketch",
    )(coupling, sketch_matrix, block_rows)


def exchange_kernel(
    sk_ref,
    owner_ref,
    pick_ref,
    own_ref,
    zbuf,
    slots,
    rbuf,
    ysend,
    gbuf,
    stage,
    obuf,
    pbuf,
    zsend,
    zrecv,
    rsend,
    rrecv,
    gsend,
    grecv,
    fsend,
    frecv,
    osend,
    orecv,
    psend,
    precv,
):
    s = lax.axis_index("sub")
    g = lax.axis_index("grp")
    core = lax.rem(s, 2)
    chip = s // 2
    y = chip // SIDE
    x = lax.rem(chip, SIDE)
    partner = s + 1 - 2 * core
    other = 1 - core

    def ahead(d):
        return lax.rem(g + d, 4)

    def behind(d):
        return lax.rem(g + 4 - d, 4)

    def chip_to(r):
        dy, dx = RING[r]
        return lax.rem(y + dy, SIDE) * SIDE + lax.rem(x + dx, SIDE)

    def chip_from(r):
        dy, dx = RING[r]
        return lax.rem(y + SIDE - dy, SIDE) * SIDE + lax.rem(x + SIDE - dx, SIDE)

    barrier = pltpu.get_barrier_semaphore()
    peers = [(s, ahead(d)) for d in range(1, 4)]
    peers += [(partner, ahead(d)) for d in range(4)]
    peers += [(chip_to(r) * 2 + core, g) for r in range(1, 16)]
    for peer in peers:
        pl.semaphore_signal(barrier, inc=1, device_id=peer, device_id_type=MESH)
    pl.semaphore_wait(barrier, len(peers))

    def remote(src, dst, send, recv, peer):
        return pltpu.make_async_remote_copy(
            src_ref=src, dst_ref=dst, send_sem=send, recv_sem=recv,
            device_id=peer, device_id_type=MESH,
        )

    def z_copy(d, away):
        return remote(
            sk_ref.at[ahead(d)], zbuf.at[core, g], zsend.at[d, away], zrecv.at[d, away],
            (partner if away else s, ahead(d)),
        )

    z_list = [(d, away) for d in (2, 1, 3) for away in (0, 1)] + [(0, 1)]
    for d, away in z_list:
        z_copy(d, away).start()
    zbuf[core, g] = sk_ref[g]
    for d, away in z_list:
        z_copy(d, away).wait()

    owners = [owner_ref[b] for b in range(16)]

    def r_copy(r):
        return remote(
            slots.at[r], rbuf.at[r], rsend.at[r], rrecv.at[r], (chip_to(r) * 2 + core, g)
        )

    for r in FAR_FIRST + [0]:
        target = chip_to(r) * 2 + core
        total = None
        for b in range(16):
            weight = jnp.where(owners[b] == target, 1.0, 0.0).astype(F32)
            term = zbuf[b // 8, (b % 8) // 2, b % 2] * weight
            total = term if total is None else total + term
        slots[r] = total
        if r:
            r_copy(r).start()
    total = slots[0]
    for r in FAR_FIRST:
        r_copy(r).wait_recv()
    for r in FAR_FIRST:
        total = total + rbuf[r]
    ysend[...] = total
    gbuf[s] = total
    own_ref[g] = total

    def g_copy(r):
        return remote(
            ysend, gbuf.at[s], gsend.at[r], grecv.at[r], (chip_to(r) * 2 + core, g)
        )

    def g_arrived(r):
        i = chip_from(r) * 2 + core
        return remote(
            ysend, gbuf.at[i], gsend.at[r], grecv.at[r], (chip_to(r) * 2 + core, g)
        )

    def f_copy(r):
        i = chip_from(r) * 2 + core
        return remote(
            ysend if r == 0 else gbuf.at[i], gbuf.at[i], fsend.at[r], frecv.at[r], (partner, g)
        )

    def o_copy(d):
        return remote(ysend, obuf.at[g], osend.at[d], orecv.at[d], (s, ahead(d)))

    for r in FAR_FIRST:
        g_copy(r).start()
    f_copy(0).start()
    for d in (2, 1, 3):
        o_copy(d).start()
    for r in NEAR_FIRST:
        g_arrived(r).wait_recv()
        f_copy(r).start()
    for r in range(16):
        f_copy(r).wait_recv()

    def p_copy(d):
        return remote(stage.at[d - 1], pbuf.at[g], psend.at[d], precv.at[d], (s, ahead(d)))

    for d in (2, 1, 3):
        for k in range(2):
            stage[d - 1, k] = gbuf[owner_ref[8 * core + 2 * ahead(d) + k]]
        p_copy(d).start()
    for k in range(2):
        pick_ref[g, k] = gbuf[owner_ref[8 * core + 2 * g + k]]
    for d in (1, 2, 3):
        o_copy(d).wait_recv()
        own_ref[behind(d)] = obuf[behind(d)]
    for d in (1, 3, 2):
        p_copy(d).wait_recv()
        pick_ref[behind(d)] = pbuf[behind(d)]
    for d in range(1, 4):
        o_copy(d).wait_send()
        p_copy(d).wait_send()
    for r in range(16):
        f_copy(r).wait_send()
        if r:
            r_copy(r).wait_send()
            g_copy(r).wait_send()


def exchange_call(sketches, owner):
    piece = (32, LANES)
    dma = pltpu.SemaphoreType.DMA
    return pl.pallas_call(
        exchange_kernel,
        out_shape=(
            jax.ShapeDtypeStruct((4, 2) + piece, F32),
            jax.ShapeDtypeStruct((4,) + piece, F32),
        ),
        in_specs=[
            pl.BlockSpec(memory_space=pltpu.VMEM),
            pl.BlockSpec(memory_space=pltpu.SMEM),
        ],
        out_specs=(
            pl.BlockSpec(memory_space=pltpu.VMEM),
            pl.BlockSpec(memory_space=pltpu.VMEM),
        ),
        scratch_shapes=[
            pltpu.VMEM((2, 4, 2) + piece, F32),
            pltpu.VMEM((16,) + piece, F32),
            pltpu.VMEM((16,) + piece, F32),
            pltpu.VMEM(piece, F32),
            pltpu.VMEM((32,) + piece, F32),
            pltpu.VMEM((3, 2) + piece, F32),
            pltpu.VMEM((4,) + piece, F32),
            pltpu.VMEM((4, 2) + piece, F32),
            dma((4, 2)),
            dma((4, 2)),
            dma((16,)),
            dma((16,)),
            dma((16,)),
            dma((16,)),
            dma((16,)),
            dma((16,)),
            dma((4,)),
            dma((4,)),
            dma((4,)),
            dma((4,)),
        ],
        compiler_params=pltpu.CompilerParams(
            collective_id=0, has_side_effects=True, vmem_limit_bytes=8 << 20
        ),
        name="exchange",
    )(sketches, owner)


def lane_spread(v, lane):
    return jnp.broadcast_to(v[:, lane : lane + 1], v.shape)


def row_spread(v, row):
    return jnp.broadcast_to(v[row : row + 1, :], v.shape)


def inverse_factors(grams):
    size = 64
    row = lax.broadcasted_iota(jnp.int32, (size, size), 0)
    col = lax.broadcasted_iota(jnp.int32, (size, size), 1)
    unit = (row == col).astype(F32)
    inner = lax.broadcasted_iota(jnp.int32, (8, LANES), 0)
    count = len(grams)
    state = []
    for gram in grams:
        wide = jnp.concatenate([gram, unit], axis=1)
        state.append([wide[8 * i : 8 * i + 8] for i in range(8)])
    scales = [[] for _ in grams]
    for p in range(8):
        panels = [
            [[lane_spread(state[a][i], 8 * p + l) for i in range(p, 8)] for l in range(8)]
            for a in range(count)
        ]
        pivots = [jnp.ones((8, LANES), F32) for _ in grams]
        for l in range(8):
            for a in range(count):
                panel = panels[a]
                pivot = row_spread(panel[l][0], l)
                pivots[a] = jnp.where(inner == l, pivot, pivots[a])
                inv = 1.0 / pivot
                times = [v * inv for v in panel[l]]
                times[0] = jnp.where(inner > l, times[0], 0.0)
                for l2 in range(l + 1, 8):
                    element = row_spread(panel[l2][0], l)
                    panel[l2] = [v - t * element for v, t in zip(panel[l2], times)]
                line = row_spread(state[a][p], l)
                for i in range(p, 8):
                    state[a][i] = state[a][i] - times[i - p] * line
        for a in range(count):
            scales[a].append(1.0 / jnp.sqrt(pivots[a]))
    return [
        jnp.concatenate([state[a][i] * scales[a][i] for i in range(8)], axis=0)[:, size:]
        for a in range(count)
    ]


def project_kernel(c_hbm, pick_ref, own_ref, rows_ref, base_ref, out_hbm, cbuf, obuf, full, part, csem, osem):
    cols = cbuf.shape[3]
    rows = cbuf.shape[2]
    wide = cols // 4
    g = lax.axis_index("grp")

    def load(k, j):
        return pltpu.make_async_copy(
            c_hbm.at[0, k, :, pl.ds(j * wide, wide)],
            cbuf.at[0, k, :, pl.ds(j * wide, wide)],
            csem.at[k, j],
        )

    for k in range(2):
        for j in range(4):
            load(k, j).start()
    half = lax.broadcasted_iota(jnp.int32, (32, LANES), 1) < 64

    grams = []
    for a in range(3):
        piece = jnp.concatenate(
            [own_ref[q] if a == 2 else pick_ref[q, a] for q in range(4)], axis=0
        )
        both = lax.dot_general(
            piece, piece, (((0,), (0,)), ((), ())),
            precision=lax.Precision.HIGHEST, preferred_element_type=F32,
        )
        grams.append(both[:64, :64] + both[64:, 64:])
        for q in range(4):
            v = piece[32 * q : 32 * q + 32]
            full[a, pl.ds(64 * q, 32, stride=2), :] = v
            full[a, pl.ds(64 * q + 1, 32, stride=2), :] = pltpu.roll(v, 64, 1)
    inverses = inverse_factors(grams)
    mine = full[2, pl.ds(pl.multiple_of(g * 64, 64), 64), :][:, :64]
    base = lax.dot_general(
        mine, inverses[2], (((1,), (1,)), ((), ())),
        precision=lax.Precision.HIGHEST, preferred_element_type=F32,
    )
    part[...] = jnp.concatenate([base, base], axis=1)
    base_ref[...] = jnp.where(
        half, part[pl.ds(0, 32, stride=2), :], part[pl.ds(1, 32, stride=2), :]
    )

    spot = lax.broadcasted_iota(jnp.int32, (64, rows), 1)
    lefts = []
    for k in range(2):
        turned = lax.dot_general(
            inverses[k], full[k][:, :64], (((1,), (1,)), ((), ())),
            precision=lax.Precision.HIGHEST, preferred_element_type=F32,
        )
        turned = jnp.where(spot < rows_ref[0, k], turned, 0.0)
        lefts.append(jnp.concatenate(split_two(turned), axis=0))

    def store(k, j):
        return pltpu.make_async_copy(
            obuf.at[k, :, pl.ds(j * wide, wide)],
            out_hbm.at[0, k, :, pl.ds(j * wide, wide)],
            osem.at[k, j],
        )

    step = 512
    for k in range(2):
        left = lefts[k]
        for j in range(4):
            load(k, j).wait()
            for n in range(j * wide, (j + 1) * wide, step):
                high, low = split_two(cbuf[0, k, :, n : n + step])
                one = jnp.dot(left, high, preferred_element_type=F32)
                two = jnp.dot(left[:64], low, preferred_element_type=F32)
                obuf[k, :, n : n + step] = one[:64] + one[64:] + two
            store(k, j).start()
    for k in range(2):
        for j in range(4):
            store(k, j).wait()


def project_call(coupling, pick, own, block_rows):
    _, _, rows, cols = coupling.shape
    return pl.pallas_call(
        project_kernel,
        out_shape=(
            jax.ShapeDtypeStruct((32, LANES), F32),
            jax.ShapeDtypeStruct((1, 2, 64, cols), F32),
        ),
        in_specs=[
            pl.BlockSpec(memory_space=pl.ANY),
            pl.BlockSpec(memory_space=pltpu.VMEM),
            pl.BlockSpec(memory_space=pltpu.VMEM),
            pl.BlockSpec(memory_space=pltpu.SMEM),
        ],
        out_specs=(
            pl.BlockSpec(memory_space=pltpu.VMEM),
            pl.BlockSpec(memory_space=pl.ANY),
        ),
        scratch_shapes=[
            pltpu.VMEM((1, 2, rows, cols), F32),
            pltpu.VMEM((2, 64, cols), F32),
            pltpu.VMEM((3, rows, LANES), F32),
            pltpu.VMEM((64, LANES), F32),
            pltpu.SemaphoreType.DMA((2, 4)),
            pltpu.SemaphoreType.DMA((2, 4)),
        ],
        compiler_params=pltpu.CompilerParams(vmem_limit_bytes=40 << 20),
        name="project",
    )(coupling, pick, own, block_rows)


def on_device(coupling, sketch_matrix, block_rows, members):
    chip = lax.axis_index("sub") // 2
    ids = 16 * chip + lax.iota(jnp.int32, 16)
    hit = members[None, :, :] == ids[:, None, None]
    index = lax.broadcasted_iota(jnp.int32, hit.shape, 1)
    owner = jnp.sum(jnp.where(hit, index, 0), axis=(1, 2))
    sketches = sketch_call(coupling, sketch_matrix, block_rows)
    pick, own = exchange_call(sketches, owner)
    bases, projections = project_call(coupling, pick, own, block_rows)
    return (bases.reshape(1, -1), projections)


def solution(mesh):
    placed = (P(("sub", "grp"), None, None, None), P(), P(("sub", "grp"), None), P())
    return jax.shard_map(
        on_device,
        mesh=mesh,
        in_specs=placed,
        out_specs=(P("sub", "grp"), P(("sub", "grp"), None, None, None)),
        check_vma=False,
    )
```

```python
import functools

import jax
import jax.numpy as jnp
from jax import lax
from jax.experimental import pallas as pl
from jax.experimental.pallas import tpu as pltpu
from jax.sharding import PartitionSpec as P

MESH = pl.DeviceIdType.MESH
F32 = jnp.float32
BF16 = jnp.bfloat16
LANES = 128
SIDE = 4
RING = [(dy, dx) for dy in range(SIDE) for dx in range(SIDE)]
FAR_FIRST = sorted(range(1, 16), key=lambda r: -sum(min(d, SIDE - d) for d in RING[r]))
NEAR_FIRST = FAR_FIRST[::-1]


def split_two(x):
    high = x.astype(BF16)
    return high, (x - high.astype(F32)).astype(BF16)


def gather_kernel(
    c_hbm,
    s_hbm,
    rows_hbm,
    members_hbm,
    pick_ref,
    own_ref,
    cbuf,
    sbuf,
    sw,
    pairs,
    rows_ref,
    mbuf,
    owned,
    sk_ref,
    zbuf,
    slots,
    rbuf,
    ysend,
    gbuf,
    stage,
    obuf,
    pbuf,
    csem,
    ssem,
    isem,
    zsend,
    zrecv,
    rsend,
    rrecv,
    gsend,
    grecv,
    fsend,
    frecv,
    osend,
    orecv,
    psend,
    precv,
):
    parts, _, part_rows, cols = cbuf.shape
    width = sbuf.shape[0]
    s = lax.axis_index("sub")
    g = lax.axis_index("grp")
    core = lax.rem(s, 2)
    chip = s // 2
    y = chip // SIDE
    x = lax.rem(chip, SIDE)
    partner = s + 1 - 2 * core

    def ahead(d):
        return lax.rem(g + d, 4)

    def behind(d):
        return lax.rem(g + 4 - d, 4)

    def turn(t):
        return lax.rem(2 + t + t // 2 - 2 * (t // 3), 4)

    def chip_to(r):
        dy, dx = RING[r]
        return lax.rem(y + dy, SIDE) * SIDE + lax.rem(x + dx, SIDE)

    def chip_from(r):
        dy, dx = RING[r]
        return lax.rem(y + SIDE - dy, SIDE) * SIDE + lax.rem(x + SIDE - dx, SIDE)

    s_copy = pltpu.make_async_copy(s_hbm, sbuf, ssem)
    s_copy.start()
    rows_copy = pltpu.make_async_copy(rows_hbm, rows_ref, isem.at[0])
    rows_copy.start()
    members_copy = pltpu.make_async_copy(members_hbm, mbuf, isem.at[1])
    members_copy.start()

    def load(t, k):
        q = ahead(turn(t))
        return pltpu.make_async_copy(
            c_hbm.at[0, k, pl.ds(q * part_rows, part_rows), :], cbuf.at[q, k], csem.at[t, k]
        )

    for t in range(2):
        for k in range(2):
            load(t, k).start()

    barrier = pltpu.get_barrier_semaphore()
    peers = [(s, ahead(d)) for d in range(1, 4)]
    peers += [(partner, ahead(d)) for d in range(4)]
    peers += [(chip_to(r) * 2 + core, g) for r in range(1, 16)]
    for peer in peers:
        pl.semaphore_signal(barrier, inc=1, device_id=peer, device_id_type=MESH)

    sw[2 * width :, :] = jnp.zeros((256 - 2 * width, cols), BF16)
    rows_copy.wait()
    members_copy.wait()
    table = mbuf[...]
    lane = lax.broadcasted_iota(jnp.int32, table.shape, 1)
    owners = [jnp.max(jnp.where(table == 16 * chip + b, lane, 0)) for b in range(16)]
    for b in range(16):
        owned[b] = owners[b]
    s_copy.wait()
    for n in range(0, cols, 1024):
        high, low = split_two(sbuf[:, n : n + 1024])
        sw[:width, n : n + 1024] = high
        sw[width : 2 * width, n : n + 1024] = low
    pl.semaphore_wait(barrier, len(peers))

    def remote(src, dst, send, recv, peer):
        return pltpu.make_async_remote_copy(
            src_ref=src, dst_ref=dst, send_sem=send, recv_sem=recv,
            device_id=peer, device_id_type=MESH,
        )

    def z_copy(t, away):
        q = ahead(turn(t))
        return remote(
            sk_ref.at[t], zbuf.at[core, g], zsend.at[t, away], zrecv.at[t, away],
            (partner if away else s, q),
        )

    def sketch(acc0, acc1):
        accs = (acc0, acc1)
        for a in accs:
            pltpu.matmul_pop(a)

        def quarter(t, carry):
            q = ahead(turn(t))
            for k in range(2):
                load(t, k).wait()

            @pl.when(t < 2)
            def _():
                for k in range(2):
                    load(t + 2, k).start()

            for j in range(cols // 512):
                for m in range(2):
                    n = (2 * j + m) * 256
                    pltpu.matmul_push_rhs(
                        sw[:, n : n + 256], staging_register=0, mxu_index=m, transpose=True
                    )
                    block = jnp.concatenate([cbuf[q, k, :, n : n + 256] for k in range(2)], axis=0)
                    high, low = split_two(block)
                    pltpu.matmul_acc_lhs(accs[m], high, load_staged_rhs=0)
                    pltpu.matmul_acc_lhs(accs[m], low)
            total = pltpu.matmul_pop(acc0)[:, :LANES] + pltpu.matmul_pop(acc1)[:, :LANES]
            total = total + pltpu.roll(total, LANES // 2, 1)
            spot = lax.broadcasted_iota(jnp.int32, (part_rows, LANES), 0) + q * part_rows
            left = lax.broadcasted_iota(jnp.int32, (part_rows // 2, LANES), 1) < LANES // 2
            for k in range(2):
                live = total[k * part_rows : (k + 1) * part_rows]
                pairs[k] = jnp.where(spot < rows_ref[0, k], live, 0.0)
                even = pairs[k, pl.ds(0, part_rows // 2, stride=2), :]
                odd = pairs[k, pl.ds(1, part_rows // 2, stride=2), :]
                sk_ref[t, k] = jnp.where(left, even, odd)
            z_copy(t, 1).start()

            @pl.when(t < 3)
            def _():
                z_copy(t, 0).start()

            return carry

        lax.fori_loop(0, parts, quarter, 0)

    pl.run_scoped(
        sketch, pltpu.ACC(0)((2 * part_rows, 256), F32), pltpu.ACC(1)((2 * part_rows, 256), F32)
    )
    zbuf[core, g] = sk_ref[3]
    for t in range(4):
        z_copy(t, 1).wait()
        if t < 3:
            z_copy(t, 0).wait()

    def r_copy(r):
        return remote(
            slots.at[r], rbuf.at[r], rsend.at[r], rrecv.at[r], (chip_to(r) * 2 + core, g)
        )

    for r in FAR_FIRST + [0]:
        target = chip_to(r) * 2 + core
        total = None
        for b in range(16):
            weight = jnp.where(owners[b] == target, 1.0, 0.0).astype(F32)
            term = zbuf[b // 8, (b % 8) // 2, b % 2] * weight
            total = term if total is None else total + term
        slots[r] = total
        if r:
            r_copy(r).start()
    total = slots[0]
    for r in FAR_FIRST:
        r_copy(r).wait_recv()
    for r in FAR_FIRST:
        total = total + rbuf[r]
    ysend[...] = total
    gbuf[s] = total
    own_ref[g] = total

    def g_copy(r):
        return remote(
            ysend, gbuf.at[s], gsend.at[r], grecv.at[r], (chip_to(r) * 2 + core, g)
        )

    def g_arrived(r):
        i = chip_from(r) * 2 + core
        return remote(
            ysend, gbuf.at[i], gsend.at[r], grecv.at[r], (chip_to(r) * 2 + core, g)
        )

    def f_copy(r):
        i = chip_from(r) * 2 + core
        return remote(
            ysend if r == 0 else gbuf.at[i], gbuf.at[i], fsend.at[r], frecv.at[r], (partner, g)
        )

    def o_copy(d):
        return remote(ysend, obuf.at[g], osend.at[d], orecv.at[d], (s, ahead(d)))

    for r in FAR_FIRST:
        g_copy(r).start()
    f_copy(0).start()
    for d in (2, 1, 3):
        o_copy(d).start()
    for r in NEAR_FIRST:
        g_arrived(r).wait_recv()
        f_copy(r).start()
    for r in range(16):
        f_copy(r).wait_recv()

    def p_copy(d):
        return remote(stage.at[d - 1], pbuf.at[g], psend.at[d], precv.at[d], (s, ahead(d)))

    for d in (2, 1, 3):
        for k in range(2):
            stage[d - 1, k] = gbuf[owned[8 * core + 2 * ahead(d) + k]]
        p_copy(d).start()
    for k in range(2):
        pick_ref[g, k] = gbuf[owned[8 * core + 2 * g + k]]
    for d in (1, 2, 3):
        o_copy(d).wait_recv()
        own_ref[behind(d)] = obuf[behind(d)]
    for d in (1, 3, 2):
        p_copy(d).wait_recv()
        pick_ref[behind(d)] = pbuf[behind(d)]
    for d in range(1, 4):
        o_copy(d).wait_send()
        p_copy(d).wait_send()
    for r in range(16):
        f_copy(r).wait_send()
        if r:
            r_copy(r).wait_send()
            g_copy(r).wait_send()


def gather_call(coupling, sketch_matrix, block_rows, members):
    piece = (32, LANES)
    dma = pltpu.SemaphoreType.DMA
    vmem = pltpu.VMEM
    width, cols = sketch_matrix.shape
    hbm = pl.BlockSpec(memory_space=pltpu.HBM)
    return pl.pallas_call(
        gather_kernel,
        out_shape=(
            jax.ShapeDtypeStruct((4, 2) + piece, F32),
            jax.ShapeDtypeStruct((4,) + piece, F32),
            vmem((4, 2, 64, cols), F32),
        ),
        in_specs=[hbm] * 4,
        out_specs=(pl.BlockSpec(memory_space=vmem),) * 3,
        scratch_shapes=[
            vmem((width, cols), F32),
            vmem((256, cols), BF16),
            vmem((2, 64, LANES), F32),
            pltpu.SMEM((1, 2), jnp.int32),
            vmem((8, 32), jnp.int32),
            pltpu.SMEM((16,), jnp.int32),
            vmem((4, 2) + piece, F32),
            vmem((2, 4, 2) + piece, F32),
            vmem((16,) + piece, F32),
            vmem((16,) + piece, F32),
            vmem(piece, F32),
            vmem((32,) + piece, F32),
            vmem((3, 2) + piece, F32),
            vmem((4,) + piece, F32),
            vmem((4, 2) + piece, F32),
            dma((4, 2)),
            dma,
            dma((2,)),
            dma((4, 2)),
            dma((4, 2)),
            dma((16,)),
            dma((16,)),
            dma((16,)),
            dma((16,)),
            dma((16,)),
            dma((16,)),
            dma((4,)),
            dma((4,)),
            dma((4,)),
            dma((4,)),
        ],
        compiler_params=pltpu.CompilerParams(
            collective_id=0, has_side_effects=True, vmem_limit_bytes=30 << 20
        ),
        name="gather",
    )(coupling, sketch_matrix, block_rows, members)


def lane_spread(v, lane):
    return jnp.broadcast_to(v[:, lane : lane + 1], v.shape)


def row_spread(v, row):
    return jnp.broadcast_to(v[row : row + 1, :], v.shape)


def inverse_factors(grams):
    size = 64
    row = lax.broadcasted_iota(jnp.int32, (size, size), 0)
    col = lax.broadcasted_iota(jnp.int32, (size, size), 1)
    unit = (row == col).astype(F32)
    inner = lax.broadcasted_iota(jnp.int32, (8, LANES), 0)
    count = len(grams)
    state = []
    for gram in grams:
        wide = jnp.concatenate([gram, unit], axis=1)
        state.append([wide[8 * i : 8 * i + 8] for i in range(8)])
    scales = [[] for _ in grams]
    for p in range(8):
        panels = [
            [[lane_spread(state[a][i], 8 * p + l) for i in range(p, 8)] for l in range(8)]
            for a in range(count)
        ]
        pivots = [jnp.ones((8, LANES), F32) for _ in grams]
        for l in range(8):
            for a in range(count):
                panel = panels[a]
                pivot = row_spread(panel[l][0], l)
                pivots[a] = jnp.where(inner == l, pivot, pivots[a])
                inv = 1.0 / pivot
                times = [v * inv for v in panel[l]]
                times[0] = jnp.where(inner > l, times[0], 0.0)
                for l2 in range(l + 1, 8):
                    element = row_spread(panel[l2][0], l)
                    panel[l2] = [v - t * element for v, t in zip(panel[l2], times)]
                line = row_spread(state[a][p], l)
                for i in range(p, 8):
                    state[a][i] = state[a][i] - times[i - p] * line
        for a in range(count):
            scales[a].append(1.0 / jnp.sqrt(pivots[a]))
    return [
        jnp.concatenate([state[a][i] * scales[a][i] for i in range(8)], axis=0)[:, size:]
        for a in range(count)
    ]


def project_kernel(
    cbuf, pick_ref, own_ref, rows_hbm, base_ref, out_hbm, obuf, full, part, rows_ref, osem, isem
):
    parts, _, part_rows, cols = cbuf.shape
    rows = parts * part_rows
    wide = cols // 4
    g = lax.axis_index("grp")
    rows_copy = pltpu.make_async_copy(rows_hbm, rows_ref, isem)
    rows_copy.start()

    half = lax.broadcasted_iota(jnp.int32, (32, LANES), 1) < 64

    grams = []
    for a in range(3):
        piece = jnp.concatenate(
            [own_ref[q] if a == 2 else pick_ref[q, a] for q in range(4)], axis=0
        )
        both = lax.dot_general(
            piece, piece, (((0,), (0,)), ((), ())),
            precision=lax.Precision.HIGHEST, preferred_element_type=F32,
        )
        grams.append(both[:64, :64] + both[64:, 64:])
        for q in range(4):
            v = piece[32 * q : 32 * q + 32]
            full[a, pl.ds(64 * q, 32, stride=2), :] = v
            full[a, pl.ds(64 * q + 1, 32, stride=2), :] = pltpu.roll(v, 64, 1)
    inverses = inverse_factors(grams)
    mine = full[2, pl.ds(pl.multiple_of(g * 64, 64), 64), :][:, :64]
    base = lax.dot_general(
        mine, inverses[2], (((1,), (1,)), ((), ())),
        precision=lax.Precision.HIGHEST, preferred_element_type=F32,
    )
    part[...] = jnp.concatenate([base, base], axis=1)
    base_ref[...] = jnp.where(
        half, part[pl.ds(0, 32, stride=2), :], part[pl.ds(1, 32, stride=2), :]
    )

    rows_copy.wait()
    spot = lax.broadcasted_iota(jnp.int32, (64, rows), 1)
    lefts = []
    for k in range(2):
        turned = lax.dot_general(
            inverses[k], full[k][:, :64], (((1,), (1,)), ((), ())),
            precision=lax.Precision.HIGHEST, preferred_element_type=F32,
        )
        turned = jnp.where(spot < rows_ref[0, k], turned, 0.0)
        lefts.append(jnp.concatenate(split_two(turned), axis=0))

    def store(k, j):
        return pltpu.make_async_copy(
            obuf.at[k, :, pl.ds(j * wide, wide)],
            out_hbm.at[0, k, :, pl.ds(j * wide, wide)],
            osem.at[k, j],
        )

    step = 512
    for k in range(2):
        left = lefts[k]
        for j in range(4):
            for n in range(j * wide, (j + 1) * wide, step):
                high, low = split_two(jnp.concatenate([cbuf[q, k, :, n : n + step] for q in range(parts)], axis=0))
                one = jnp.dot(left, high, preferred_element_type=F32)
                two = jnp.dot(left[:64], low, preferred_element_type=F32)
                obuf[k, :, n : n + step] = one[:64] + one[64:] + two
            store(k, j).start()
    for k in range(2):
        for j in range(4):
            store(k, j).wait()


def project_call(held, pick, own, block_rows):
    parts, _, part_rows, cols = held.shape
    vmem = pltpu.VMEM
    spec = pl.BlockSpec(memory_space=vmem)
    hbm = pl.BlockSpec(memory_space=pltpu.HBM)
    return pl.pallas_call(
        project_kernel,
        out_shape=(
            jax.ShapeDtypeStruct((32, LANES), F32),
            jax.ShapeDtypeStruct((1, 2, 64, cols), F32),
        ),
        in_specs=[spec, spec, spec, hbm],
        out_specs=(spec, hbm),
        scratch_shapes=[
            vmem((2, 64, cols), F32),
            vmem((3, parts * part_rows, LANES), F32),
            vmem((64, LANES), F32),
            pltpu.SMEM((1, 2), jnp.int32),
            pltpu.SemaphoreType.DMA((2, 4)),
            pltpu.SemaphoreType.DMA,
        ],
        compiler_params=pltpu.CompilerParams(vmem_limit_bytes=30 << 20),
        name="project",
    )(held, pick, own, block_rows)


def on_device(coupling, sketch_matrix, block_rows, members):
    hbm = [
        pltpu.with_memory_space_constraint(v, pltpu.HBM)
        for v in (coupling, sketch_matrix, block_rows, members.T)
    ]
    pick, own, held = gather_call(*hbm)
    bases, projections = project_call(held, pick, own, hbm[2])
    return (bases.reshape(1, -1), projections)


def solution(mesh):
    placed = (P(("sub", "grp"), None, None, None), P(), P(("sub", "grp"), None), P())
    return jax.shard_map(
        on_device,
        mesh=mesh,
        in_specs=placed,
        out_specs=(P("sub", "grp"), P(("sub", "grp"), None, None, None)),
        check_vma=False,
    )
```

```python
import jax
import jax.numpy as jnp
from jax import lax
from jax.experimental import pallas as pl
from jax.experimental.pallas import tpu as pltpu
from jax.sharding import PartitionSpec as P

MESH = pl.DeviceIdType.MESH
F32 = jnp.float32
BF16 = jnp.bfloat16
LANES = 128
SIDE = 4
RING = [(dy, dx) for dy in range(SIDE) for dx in range(SIDE)]
FAR_FIRST = sorted(range(1, 16), key=lambda r: -sum(min(d, SIDE - d) for d in RING[r]))
NEAR_FIRST = FAR_FIRST[::-1]
PIECES = 4


def split_two(x):
    high = x.astype(BF16)
    return high, (x - high.astype(F32)).astype(BF16)


def split_three(x):
    high = x.astype(BF16)
    rest = x - high.astype(F32)
    middle = rest.astype(BF16)
    return high, middle, (rest - middle.astype(F32)).astype(BF16)


def on_left(shape):
    return lax.broadcasted_iota(jnp.int32, shape, 1) < LANES // 2


def half_turn(v):
    return pltpu.roll(v, LANES // 2, 1)


def lane_spread(v, lane):
    return jnp.broadcast_to(v[:, lane : lane + 1], v.shape)


def row_spread(v, row):
    return jnp.broadcast_to(v[row : row + 1, :], v.shape)


def unpack_rows(piece, store):
    turned = half_turn(piece)
    left = on_left(piece.shape)
    count = piece.shape[0]
    store[pl.ds(0, count, stride=2), :] = jnp.where(left, piece, turned)
    store[pl.ds(1, count, stride=2), :] = jnp.where(left, turned, piece)


def gram_of(rows, turned, acc, mxu):
    high, middle, low = split_three(rows)
    left = on_left(rows.shape)
    right = jnp.concatenate(
        [jnp.where(left, high, middle), jnp.where(left, low, jnp.zeros_like(low))], axis=1
    )
    pltpu.matmul_push_rhs(right, staging_register=0, mxu_index=mxu)
    pltpu.matmul_acc_lhs(acc, jnp.concatenate(split_three(turned), axis=0), load_staged_rhs=0)

    def finish():
        out = pltpu.matmul_pop(acc)
        total = (out[128:192] + out[64:128]) + out[:64]
        total = total[:, LANES:] + total[:, :LANES]
        return total + half_turn(total)

    return finish


def inverse_pair(gram, between):
    left = on_left((8, LANES))
    inner = lax.broadcasted_iota(jnp.int32, (8, LANES), 0)
    lane = lax.rem(lax.broadcasted_iota(jnp.int32, (8, LANES), 1), 64)
    a = [gram[8 * i : 8 * i + 8] for i in range(8)]
    b = [(lane == inner + 8 * i).astype(F32) for i in range(8)]
    scales = []
    for p in range(8):
        panel = [
            [
                jnp.where(left, lane_spread(a[i], 8 * p + l), lane_spread(a[i], 64 + 8 * p + l))
                for i in range(p, 8)
            ]
            for l in range(8)
        ]
        pivots = jnp.ones((8, LANES), F32)
        for l in range(8):
            pivot = row_spread(panel[l][0], l)
            pivots = jnp.where(inner == l, pivot, pivots)
            inv = 1.0 / pivot
            times = [v * inv for v in panel[l]]
            times[0] = jnp.where(inner > l, times[0], 0.0)
            for l2 in range(l + 1, 8):
                element = row_spread(panel[l2][0], l)
                panel[l2] = [v - t * element for v, t in zip(panel[l2], times)]
            line_a, line_b = row_spread(a[p], l), row_spread(b[p], l)
            for i in range(p, 8):
                if p < 7:
                    a[i] = a[i] - times[i - p] * line_a
                b[i] = b[i] - times[i - p] * line_b
            between()
        scales.append(1.0 / jnp.sqrt(pivots))
    return jnp.concatenate([v * c for v, c in zip(b, scales)], axis=0)


def twice_split(v):
    high, low = split_two(v)
    once = jnp.where(on_left(v.shape), high, low)
    return jnp.concatenate([once, once], axis=1)


def gather_kernel(
    c_hbm,
    s_hbm,
    rows_hbm,
    members_hbm,
    pick_ref,
    base_ref,
    high_ref,
    low_ref,
    cbuf,
    sbuf,
    sw,
    pairs,
    rows_ref,
    mbuf,
    ownv,
    owned,
    sk_ref,
    zbuf,
    slots,
    rbuf,
    ysend,
    gbuf,
    stage,
    obuf,
    pbuf,
    full,
    firstsem,
    csem,
    isem,
    zsend,
    zrecv,
    rsend,
    rrecv,
    gsend,
    grecv,
    fsend,
    frecv,
    osend,
    orecv,
    psend,
    precv,
):
    parts, _, part_rows, cols = cbuf.shape
    width = sbuf.shape[0]
    piece = cols // PIECES
    s = lax.axis_index("sub")
    g = lax.axis_index("grp")
    core = lax.rem(s, 2)
    chip = s // 2
    y = chip // SIDE
    x = lax.rem(chip, SIDE)
    partner = s + 1 - 2 * core

    def ahead(d):
        return lax.rem(g + d, 4)

    def behind(d):
        return lax.rem(g + 4 - d, 4)

    def turn(t):
        return lax.rem(2 + t + t // 2 - 2 * (t // 3), 4)

    def chip_to(r):
        dy, dx = RING[r]
        return lax.rem(y + dy, SIDE) * SIDE + lax.rem(x + dx, SIDE)

    def chip_from(r):
        dy, dx = RING[r]
        return lax.rem(y + SIDE - dy, SIDE) * SIDE + lax.rem(x + SIDE - dx, SIDE)

    def remote(src, dst, send, recv, peer):
        return pltpu.make_async_remote_copy(
            src_ref=src, dst_ref=dst, send_sem=send, recv_sem=recv,
            device_id=peer, device_id_type=MESH,
        )

    def first_loads(i):
        span = pl.ds(i * piece, piece)
        q = ahead(turn(0))
        loads = [pltpu.make_async_copy(s_hbm.at[:, span], sbuf.at[:, span], firstsem.at[3 * i])]
        for k in range(2):
            loads.append(
                pltpu.make_async_copy(
                    c_hbm.at[0, k, pl.ds(q * part_rows, part_rows), span],
                    cbuf.at[q, k, :, span],
                    firstsem.at[3 * i + 1 + k],
                )
            )
        return loads

    def load(t, k):
        q = ahead(turn(t))
        return pltpu.make_async_copy(
            c_hbm.at[0, k, pl.ds(q * part_rows, part_rows), :], cbuf.at[q, k], csem.at[t, k]
        )

    for i in range(PIECES):
        for copy in first_loads(i):
            copy.start()
    rows_copy = pltpu.make_async_copy(rows_hbm, rows_ref, isem.at[0])
    rows_copy.start()
    members_copy = pltpu.make_async_copy(members_hbm, mbuf, isem.at[1])
    members_copy.start()
    for k in range(2):
        load(1, k).start()

    barrier = pltpu.get_barrier_semaphore()
    peers = [(s, ahead(d)) for d in range(1, 4)]
    peers += [(partner, ahead(d)) for d in range(4)]
    peers += [(chip_to(r) * 2 + core, g) for r in range(1, 16)]
    for peer in peers:
        pl.semaphore_signal(barrier, inc=1, device_id=peer, device_id_type=MESH)

    def z_copy(t, away):
        return remote(
            sk_ref.at[t], zbuf.at[4 * core + g], zsend, zrecv,
            (partner if away else s, ahead(turn(t))),
        )

    def work(acc0, acc1, gacc, bacc):
        accs = (acc0, acc1)
        for a in (acc0, acc1, gacc, bacc):
            pltpu.matmul_pop(a)
        sw[2 * width :, :] = jnp.zeros((256 - 2 * width, cols), BF16)

        def products(q, start, stop):
            for n in range(start, stop, 256):
                m = n // 256 % 2
                pltpu.matmul_push_rhs(
                    sw[:, n : n + 256], staging_register=0, mxu_index=m, transpose=True
                )
                halves = [split_two(cbuf[q, k, :, n : n + 256]) for k in range(2)]
                for k in range(2):
                    high_ref[q, k, :, n : n + 256] = halves[k][0]
                    low_ref[q, k, :, n : n + 256] = halves[k][1]
                for i in range(2):
                    pltpu.matmul_acc_lhs(
                        accs[m],
                        jnp.concatenate([halves[0][i], halves[1][i]], axis=0),
                        load_staged_rhs=None if i else 0,
                    )

        def finish(t, q):
            total = pltpu.matmul_pop(acc0)[:, :LANES] + pltpu.matmul_pop(acc1)[:, :LANES]
            total = total + half_turn(total)
            spot = lax.broadcasted_iota(jnp.int32, (part_rows, LANES), 0) + q * part_rows
            left = on_left((part_rows // 2, LANES))
            for k in range(2):
                live = total[k * part_rows : (k + 1) * part_rows]
                pairs[k] = jnp.where(spot < rows_ref[0, k], live, 0.0)
                even = pairs[k, pl.ds(0, part_rows // 2, stride=2), :]
                odd = pairs[k, pl.ds(1, part_rows // 2, stride=2), :]
                sk_ref[t, k] = jnp.where(left, even, odd)

        q0 = ahead(turn(0))
        for i in range(PIECES):
            span = slice(i * piece, (i + 1) * piece)
            for copy in first_loads(i):
                copy.wait()
            high, low = split_two(sbuf[:, span])
            sw[:width, span] = high
            sw[width : 2 * width, span] = low
            products(q0, i * piece, (i + 1) * piece)
        for k in range(2):
            load(2, k).start()
        rows_copy.wait()
        finish(0, q0)
        pl.semaphore_wait(barrier, len(peers))
        z_copy(0, 1).start()
        z_copy(0, 0).start()

        members_copy.wait()
        table = mbuf[...]
        lane = lax.broadcasted_iota(jnp.int32, table.shape, 1)
        found = jnp.concatenate(
            [
                jnp.max(jnp.where(table == 16 * chip + b, lane, 0), axis=0, keepdims=True)
                for b in range(16)
            ],
            axis=0,
        )
        ownv[...] = jnp.broadcast_to(jnp.max(found, axis=1, keepdims=True), ownv.shape)
        own_copy = pltpu.make_async_copy(ownv, owned, isem.at[2])
        own_copy.start()

        def quarter(t, carry):
            q = ahead(turn(t))
            for k in range(2):
                load(t, k).wait()

            @pl.when(t < 2)
            def _():
                for k in range(2):
                    load(t + 2, k).start()

            products(q, 0, cols)
            finish(t, q)
            z_copy(t, 1).start()

            @pl.when(t < 3)
            def _():
                z_copy(t, 0).start()

            return carry

        lax.fori_loop(1, parts, quarter, 0)
        own_copy.wait()
        zbuf[4 * core + g] = sk_ref[3]

        def z_all():
            return remote(
                zbuf.at[pl.ds(0, 7)], zbuf.at[pl.ds(0, 7)], zsend, zrecv, (partner, g)
            )

        z_all().wait_recv()
        owners = [owned[b, 0] for b in range(16)]

        def r_copy(r):
            return remote(slots.at[r], rbuf.at[r], rsend, rrecv, (chip_to(r) * 2 + core, g))

        def r_all():
            return remote(
                rbuf.at[pl.ds(1, 15)], rbuf.at[pl.ds(1, 15)], rsend, rrecv, (partner, g)
            )

        for r in FAR_FIRST + [0]:
            target = chip_to(r) * 2 + core
            total = None
            for b in range(16):
                weight = jnp.where(owners[b] == target, 1.0, 0.0).astype(F32)
                term = zbuf[b // 2, b % 2] * weight
                total = term if total is None else total + term
            slots[r] = total
            if r:
                r_copy(r).start()
        total = slots[0]
        r_all().wait_recv()
        for r in FAR_FIRST:
            total = total + rbuf[r]
        ysend[...] = total
        gbuf[s] = total
        obuf[g] = total

        def g_copy(r, i):
            return remote(
                ysend, gbuf.at[i], gsend, grecv.at[r], (chip_to(r) * 2 + core, g)
            )

        def f_copy(r):
            i = chip_from(r) * 2 + core
            return remote(
                ysend if r == 0 else gbuf.at[i], gbuf.at[i], fsend, frecv, (partner, g)
            )

        def f_all():
            return remote(
                gbuf.at[pl.ds(0, 16)], gbuf.at[pl.ds(0, 16)], fsend, frecv, (partner, g)
            )

        def o_copy(d):
            return remote(ysend, obuf.at[g], osend, orecv, (s, ahead(d)))

        def o_all():
            return remote(obuf.at[pl.ds(0, 3)], obuf.at[pl.ds(0, 3)], osend, orecv, (partner, g))

        for r in FAR_FIRST:
            g_copy(r, s).start()
        f_copy(0).start()
        for d in (2, 1, 3):
            o_copy(d).start()
        for r in NEAR_FIRST:
            g_copy(r, chip_from(r) * 2 + core).wait_recv()
            f_copy(r).start()
        f_all().wait_recv()

        def p_copy(d):
            return remote(stage.at[d - 1], pbuf.at[g], psend, precv, (s, ahead(d)))

        def p_all():
            return remote(pbuf.at[pl.ds(0, 3)], pbuf.at[pl.ds(0, 3)], psend, precv, (partner, g))

        for d in (2, 1, 3):
            for k in range(2):
                stage[d - 1, k] = gbuf[owned[8 * core + 2 * ahead(d) + k, 0]]
            p_copy(d).start()
        for k in range(2):
            pbuf[g, k] = gbuf[owned[8 * core + 2 * g + k, 0]]

        o_all().wait_recv()
        for q in range(parts):
            unpack_rows(obuf[q], full.at[pl.ds(q * part_rows, part_rows)])
        rows = full[...]
        gram = gram_of(rows, rows.T[:64], gacc, 0)()
        inverse = inverse_pair(gram, lambda: None)
        mine = full[pl.ds(pl.multiple_of(g * part_rows, part_rows), part_rows), :]
        spread = jnp.concatenate(
            [twice_split(inverse), jnp.zeros((192, 256), BF16)], axis=0
        )
        pltpu.matmul_push_rhs(spread, staging_register=0, mxu_index=1, transpose=True)
        pltpu.matmul_acc_lhs(bacc, jnp.concatenate(split_two(mine), axis=1), load_staged_rhs=0)
        base = pltpu.matmul_pop(bacc)[:, :LANES]
        base = jnp.where(on_left(base.shape), base, half_turn(base))
        pairs[0] = base
        base_ref[...] = jnp.where(
            on_left((32, LANES)),
            pairs[0, pl.ds(0, 32, stride=2), :],
            pairs[0, pl.ds(1, 32, stride=2), :],
        )
        p_all().wait_recv()
        pick_ref[...] = pbuf[...]
        z_all().wait_send()
        r_all().wait_send()
        remote(
            gbuf.at[pl.ds(0, 15)], gbuf.at[pl.ds(0, 15)], gsend, grecv.at[0], (partner, g)
        ).wait_send()
        f_all().wait_send()
        o_all().wait_send()
        p_all().wait_send()

    pl.run_scoped(
        work,
        pltpu.ACC(0)((2 * part_rows, 256), F32),
        pltpu.ACC(1)((2 * part_rows, 256), F32),
        pltpu.ACC(0)((192, 256), F32),
        pltpu.ACC(1)((64, 256), F32),
    )


def gather_call(coupling, sketch_matrix, block_rows, members):
    piece = (32, LANES)
    dma = pltpu.SemaphoreType.DMA
    vmem = pltpu.VMEM
    width, cols = sketch_matrix.shape
    return pl.pallas_call(
        gather_kernel,
        out_shape=(
            jax.ShapeDtypeStruct((4, 2) + piece, F32),
            jax.ShapeDtypeStruct(piece, F32),
            vmem((4, 2, 64, cols), BF16),
            vmem((4, 2, 64, cols), BF16),
        ),
        in_specs=[pl.BlockSpec(memory_space=pltpu.HBM)] * 4,
        out_specs=(pl.BlockSpec(memory_space=vmem),) * 4,
        scratch_shapes=[
            vmem((4, 2, 64, cols), F32),
            vmem((width, cols), F32),
            vmem((256, cols), BF16),
            vmem((2, 64, LANES), F32),
            pltpu.SMEM((1, 2), jnp.int32),
            vmem((8, 32), jnp.int32),
            vmem((16, LANES), jnp.int32),
            pltpu.SMEM((16, LANES), jnp.int32),
            vmem((4, 2) + piece, F32),
            vmem((8, 2) + piece, F32),
            vmem((16,) + piece, F32),
            vmem((16,) + piece, F32),
            vmem(piece, F32),
            vmem((32,) + piece, F32),
            vmem((3, 2) + piece, F32),
            vmem((4,) + piece, F32),
            vmem((4, 2) + piece, F32),
            vmem((256, LANES), F32),
            dma((3 * PIECES,)),
            dma((4, 2)),
            dma((3,)),
            dma,
            dma,
            dma,
            dma,
            dma,
            dma((16,)),
            dma,
            dma,
            dma,
            dma,
            dma,
            dma,
        ],
        compiler_params=pltpu.CompilerParams(
            collective_id=0, has_side_effects=True, vmem_limit_bytes=29 << 20
        ),
        name="gather",
    )(coupling, sketch_matrix, block_rows, members)


def project_kernel(high_ref, low_ref, pick_ref, base_in, rows_hbm, base_ref, out_hbm, obuf, wbuf, full, rows_ref, osem, isem):
    parts, _, part_rows, cols = high_ref.shape
    count = parts * part_rows
    rows_copy = pltpu.make_async_copy(rows_hbm, rows_ref, isem)
    rows_copy.start()
    base_ref[...] = base_in[...]

    def work(*accs):
        grams, wides = accs[:2], accs[2:]
        for a in accs:
            pltpu.matmul_pop(a)
        for k in range(2):
            for q in range(parts):
                unpack_rows(pick_ref[q, k], full.at[k, pl.ds(q * part_rows, part_rows)])
        rows = [full[k] for k in range(2)]
        turned = [v.T[:64] for v in rows]
        ends = [gram_of(rows[k], turned[k], grams[k], k) for k in range(2)]
        rows_copy.wait()
        spot = lax.broadcasted_iota(jnp.int32, (64, count), 1)
        lefts = [
            split_two(jnp.where(spot < rows_ref[0, k], turned[k], 0.0)) for k in range(2)
        ]
        left = on_left((64, LANES))
        gram = jnp.where(left, ends[0](), ends[1]())

        tiles = [(k, n) for k in range(2) for n in range(0, cols, 256)]
        used = [0]

        def accumulator(m):
            used[0] += 1
            pool = wides[m::2]
            return pool[used[0] // 2 % len(pool)]

        waiting = []

        def collect():
            k, n, acc = waiting.pop(0)
            high, low = split_two(pltpu.matmul_pop(acc))
            wbuf[0, k, :, n : n + 256] = high
            wbuf[1, k, :, n : n + 256] = low

        todo = list(tiles)

        def between():
            if not todo:
                return
            k, n = todo.pop(0)
            m = n // 256 % 2
            acc = accumulator(m)
            for i, ref in enumerate((high_ref, low_ref)):
                tile = jnp.concatenate([ref[q, k, :, n : n + 256] for q in range(parts)], axis=0)
                pltpu.matmul_push_rhs(tile, staging_register=i, mxu_index=m)
                pltpu.matmul_acc_lhs(acc, lefts[k][0], load_staged_rhs=i)
                if i == 0:
                    pltpu.matmul_acc_lhs(acc, lefts[k][1])
            waiting.append((k, n, acc))
            if len(waiting) > 4:
                collect()

        both = inverse_pair(gram, between)
        while todo:
            between()
        while waiting:
            collect()
        other = half_turn(both)
        inverses = [jnp.where(left, both, other), jnp.where(left, other, both)]
        stacks = [twice_split(v) for v in inverses]

        def store(k, n, size):
            return pltpu.make_async_copy(
                obuf.at[k, :, pl.ds(n, size)], out_hbm.at[0, k, :, pl.ds(n, size)], osem
            )

        def put():
            k, n, acc = waiting.pop(0)
            obuf[k, :, n : n + 256] = pltpu.matmul_pop(acc)
            if n % 1024 == 768:
                store(k, n - 768, 1024).start()

        for k, n in tiles:
            m = n // 256 % 2
            acc = accumulator(m)
            high, low = wbuf[0, k, :, n : n + 256], wbuf[1, k, :, n : n + 256]
            pltpu.matmul_push_rhs(
                jnp.concatenate([high, high, low, low], axis=0), staging_register=0, mxu_index=m
            )
            pltpu.matmul_acc_lhs(acc, stacks[k], load_staged_rhs=0)
            waiting.append((k, n, acc))
            if len(waiting) > 4:
                put()
        while waiting:
            put()
        pltpu.make_async_copy(obuf, out_hbm.at[0], osem).wait()

    pl.run_scoped(
        work,
        pltpu.ACC(0)((192, 256), F32),
        pltpu.ACC(1)((192, 256), F32),
        *[pltpu.ACC(i % 2)((64, 256), F32) for i in range(16)],
    )


def project_call(high, low, pick, base, block_rows):
    parts, _, part_rows, cols = high.shape
    vmem = pltpu.VMEM
    spec = pl.BlockSpec(memory_space=vmem)
    hbm = pl.BlockSpec(memory_space=pltpu.HBM)
    return pl.pallas_call(
        project_kernel,
        out_shape=(
            jax.ShapeDtypeStruct((32, LANES), F32),
            jax.ShapeDtypeStruct((1, 2, 64, cols), F32),
        ),
        in_specs=[spec, spec, spec, spec, hbm],
        out_specs=(spec, hbm),
        scratch_shapes=[
            vmem((2, 64, cols), F32),
            vmem((2, 2, 64, cols), BF16),
            vmem((2, parts * part_rows, LANES), F32),
            pltpu.SMEM((1, 2), jnp.int32),
            pltpu.SemaphoreType.DMA,
            pltpu.SemaphoreType.DMA,
        ],
        compiler_params=pltpu.CompilerParams(vmem_limit_bytes=29 << 20),
        name="project",
    )(high, low, pick, base, block_rows)


def on_device(coupling, sketch_matrix, block_rows, members):
    hbm = [
        pltpu.with_memory_space_constraint(v, pltpu.HBM)
        for v in (coupling, sketch_matrix, block_rows, members.T)
    ]
    pick, base, high, low = gather_call(*hbm)
    bases, projections = project_call(high, low, pick, base, hbm[2])
    return (bases.reshape(1, -1), projections)


def solution(mesh):
    placed = (P(("sub", "grp"), None, None, None), P(), P(("sub", "grp"), None), P())
    return jax.shard_map(
        on_device,
        mesh=mesh,
        in_specs=placed,
        out_specs=(P("sub", "grp"), P(("sub", "grp"), None, None, None)),
        check_vma=False,
    )
```
